32 devices in a mesh: pair: 8 (over z, y), aux: 4 (over x, core).
Axes of the slice: x: 2, y: 2, z: 4, core: 2. Of those that a mesh axis runs over, the one named last changes fastest.
Arguments:
- ints_ac: bfloat16 [192, 512, 4096], P(None, ('pair', 'aux')), may hold values from -0.375 to 0.375
- slot_pair: int32 [192], replicated, may hold values from 0 to 191, each once
- amplitudes: bfloat16 [192, 2, 4096], P(('pair', 'aux')), may hold values from -6 to 6
- ranks: int32 [192], P(('pair', 'aux')), may hold values from 16 to 64
- pair_occ: int32 [192, 2], P(('pair', 'aux')), may hold values from 0 to 47
- pno_energy: float32 [192, 64], P(('pair', 'aux')), may hold values from 0.2 to 3
- occ_energy: float32 [48], replicated, may hold values from -2 to -0.3
Outputs:
- ext_residual: float32 [192, 2, 4096], P(('pair', 'aux'))
- new_amplitudes: bfloat16 [192, 2, 4096], P(('pair', 'aux'))
The draws below stay inside these ranges and needn't reach their ends.
Inputs may be any that keep to these rules, and one draw needn't show every extreme that they name: `slot_pair`: a permutation of the pairs. Entries a >= ranks[s] of a slot's blocks are padding.
All inputs are finite; a program needn't handle non-finite values.
Results may differ from the reference program's by a relative error of at most 0.0039.
Values may be sent and summed in bfloat16 or wider, within the bound.
A program may use at most 128 MiB of HBM per device.

```python
import jax
import jax.numpy as jnp
from jax import lax

RANK = 64
NAUX = 512
NOCC = 48
PAIRS = 192


def plant(entries, own_key, low, largest):
    longest = entries.shape.index(max(entries.shape))
    spots = []
    for shift in (0, 1):
        where = [jax.random.randint(jax.random.fold_in(own_key, axis), (), 0, length) for axis, length in enumerate(entries.shape)]
        where[longest] = (where[longest] + shift) % entries.shape[longest]
        spots.append(tuple(where))
    return entries.at[spots[0]].set(low).at[spots[1]].set(largest)


def block_scale(rng, dims, pieces, low, top_value):
    level, own = 1.0, jax.random.fold_in(rng, 6)
    for dim, blocks in pieces:
        heights = jnp.exp(jax.random.uniform(jax.random.fold_in(own, dim), (blocks,), jnp.float32, low / len(pieces), top_value / len(pieces)))
        level = level * jnp.repeat(heights, dims[dim] // blocks).reshape([-1 if axis == dim else 1 for axis in range(len(dims))])
    return level


def normal_values(stream_key, extent, spread, most, cuts=(), kind=jnp.bfloat16):
    factor_of = block_scale(stream_key, extent, cuts, -0.22, 0.18) if cuts else 1.0
    array = jax.random.normal(stream_key, extent, jnp.float32) * spread * factor_of
    return jnp.minimum(jnp.maximum(array, -most), most).astype(kind)


def setup_inputs(seed: int = 0) -> dict:
    key_list = jax.random.split(jax.random.key(seed), 8)
    return {
        "ints_ac": normal_values(key_list[0], (PAIRS, NAUX, RANK * RANK), ((NAUX * RANK * RANK) ** -0.25), 0.375, ((1, 32),)),
        "slot_pair": jax.random.permutation(key_list[1], PAIRS).astype(jnp.int32),
        "amplitudes": normal_values(key_list[2], (PAIRS, 2, RANK * RANK), 1.0, 6.0, ((0, 32),)),
        "ranks": plant(jax.random.randint(key_list[3], (PAIRS,), RANK // 4, RANK + 1), jax.random.fold_in(key_list[3], 1), RANK // 4, RANK).astype(jnp.int32),
        "pair_occ": plant(jax.random.randint(key_list[4], (PAIRS, 2), 0, NOCC), jax.random.fold_in(key_list[4], 1), 0, NOCC - 1).astype(jnp.int32),
        "pno_energy": jnp.clip(0.2 + 2.8 * jax.random.uniform(key_list[5], (PAIRS, RANK), jnp.float32) ** block_scale(key_list[5], (PAIRS, RANK), ((0, 32),), -0.2, 0.2), 0.2, 3.0),
        "occ_energy": jnp.clip(jax.random.uniform(key_list[6], (NOCC,), jnp.float32, -2.0, -0.3), -2.0, -0.3),
    }


def reference(ints_ac, slot_pair, amplitudes, ranks, pair_occ, pno_energy, occ_energy):
    positions = jnp.arange(RANK, dtype=jnp.int32)
    masks = (positions[None, :] < ranks[:, None]).astype(jnp.float32)

    def one_slot(slot):
        pair_index = slot_pair[slot].astype(jnp.int32)
        block = lax.dynamic_index_in_dim(ints_ac, pair_index, 0, keepdims=False)
        amps = lax.dynamic_index_in_dim(amplitudes, slot, 0, keepdims=False)
        mask = lax.dynamic_index_in_dim(masks, slot, 0, keepdims=False)
        square = (mask[:, None] * mask[None, :]).reshape(RANK * RANK).astype(jnp.bfloat16)
        masked_b = (block * square).reshape(NAUX, RANK, RANK).astype(jnp.float32)
        masked_t = (amps * square).reshape(2, RANK, RANK).astype(jnp.float32)
        inner = jnp.einsum("pac,kcd->pakd", masked_b, masked_t).astype(jnp.bfloat16).astype(jnp.float32)
        result = jnp.einsum("pakd,pbd->kab", inner, masked_b)
        return result.reshape(2, RANK * RANK)

    ext_residual = lax.map(one_slot, jnp.arange(PAIRS, dtype=jnp.int32))
    occ_pair = occ_energy[pair_occ]
    denom = pno_energy[:, :, None] + pno_energy[:, None, :] - (occ_pair[:, 0] + occ_pair[:, 1])[:, None, None]
    square = masks[:, :, None] * masks[:, None, :]
    masked_t = amplitudes.astype(jnp.float32).reshape(PAIRS, 2, RANK, RANK) * square[:, None]
    updated = (masked_t - ext_residual.reshape(PAIRS, 2, RANK, RANK) / denom[:, None]) * square[:, None]
    new_amplitudes = updated.reshape(PAIRS, 2, RANK * RANK).astype(jnp.bfloat16)
    return ext_residual, new_amplitudes
```

```python
import functools

import jax
import jax.numpy as jnp
from jax import lax
from jax.experimental import pallas as pl
from jax.experimental.pallas import tpu as pltpu
from jax.sharding import PartitionSpec as P

GROUP = 8


def exchange_kernel(group, width, order_ref, *refs):
    blocks, amps_ref, out_ref, rows_ref = refs[:group], refs[group], refs[group + 1], refs[group + 2]
    lanes = 2 * width
    aux = blocks[0].shape[1]
    chunks = width * width // lanes
    half_t = lax.broadcasted_iota(jnp.int32, (width, lanes), 1) < width
    half_b = lax.broadcasted_iota(jnp.int32, (chunks, lanes), 1) < width
    for slot in range(group):
        block = blocks[slot]
        for chunk in range(chunks):
            rows_ref[slot, pl.ds(chunk * aux, aux), :] = block[
                0, :, pl.ds(chunk * lanes, lanes)
            ].astype(jnp.float32)
        pieces = []
        for pair in range(aux // 2):
            first = rows_ref[slot, pl.ds(2 * pair, chunks, stride=aux), :]
            second = rows_ref[slot, pl.ds(2 * pair + 1, chunks, stride=aux), :]
            even = jnp.where(half_b, first, pltpu.roll(second, width, 1))
            odd = jnp.where(half_b, pltpu.roll(first, width, 1), second)
            pieces.append(jnp.concatenate([even, odd], axis=0).astype(jnp.bfloat16))
        stacked = jnp.concatenate(pieces, axis=0)
        amps = amps_ref[slot].astype(jnp.float32)
        turned = pltpu.roll(amps, width, 1)
        none = jnp.zeros_like(amps)
        weights = jnp.concatenate(
            [
                jnp.concatenate([jnp.where(half_t, amps, none), jnp.where(half_t, none, turned)], axis=0),
                jnp.concatenate([jnp.where(half_t, turned, none), jnp.where(half_t, none, amps)], axis=0),
            ],
            axis=1,
        ).astype(jnp.bfloat16)
        inner = jnp.dot(stacked, weights, preferred_element_type=jnp.float32).astype(jnp.bfloat16)
        left = jnp.concatenate(pieces, axis=1)
        right = jnp.concatenate(
            [
                jnp.concatenate(
                    [
                        inner[pair * width : (pair + 1) * width, k * lanes : (k + 1) * lanes]
                        for pair in range(aux // 2)
                    ],
                    axis=1,
                )
                for k in range(2)
            ],
            axis=0,
        )
        out_ref[slot] = lax.dot_general(
            left, right, (((1,), (1,)), ((), ())), preferred_element_type=jnp.float32
        ).astype(out_ref.dtype)


def partials(ints_ac, slot_pair, amps):
    count, width, lanes = amps.shape
    aux = ints_ac.shape[1]
    group = max(g for g in range(1, GROUP + 1) if count % g == 0)

    def block_map(offset):
        return lambda step, order: (order[step * group + offset], 0, 0)

    return pl.pallas_call(
        lambda *refs: exchange_kernel(group, width, *refs),
        grid_spec=pltpu.PrefetchScalarGridSpec(
            num_scalar_prefetch=1,
            grid=(count // group,),
            in_specs=[
                pl.BlockSpec((1, aux, width * width), block_map(offset)) for offset in range(group)
            ]
            + [pl.BlockSpec((group, width, lanes), lambda step, order: (step, 0, 0))],
            out_specs=pl.BlockSpec((group, width, lanes), lambda step, order: (step, 0, 0)),
            scratch_shapes=[pltpu.VMEM((group, aux * width // 2, lanes), jnp.float32)],
        ),
        out_shape=jax.ShapeDtypeStruct((count, width, lanes), jnp.bfloat16),
        cost_estimate=pl.CostEstimate(
            flops=8 * count * aux * width**3,
            bytes_accessed=ints_ac.size * 2 + amps.size * 4,
            transcendentals=0,
        ),
        name="exchange",
    )(slot_pair, *([ints_ac] * group), amps)


def layout_of(pairs, aux):
    side = aux // 2
    if pairs % side:
        side = 1
    return pairs // side, side, aux // side // 2


class Place:
    def __init__(self, pairs, aux):
        self.deep, self.side, _ = layout_of(pairs, aux)
        pair, lane = lax.axis_index("pair"), lax.axis_index("aux")
        self.z, self.y = pair // self.side, pair % self.side
        self.x, self.core = lane // 2, lane % 2

    def spot(self, dz, i, j):
        z = (self.z + dz) % self.deep
        y = (self.y + i * (1 - self.core) + j * self.core) % self.side
        x = (self.x + j * (1 - self.core) + i * self.core) % self.side
        return z, y, x

    def block(self, dz, i, j):
        z, y, x = self.spot(dz, i, j)
        return ((z * self.side + y) * self.side + x) * 2 + self.core

    def device(self, dz, i, j):
        z, y, x = self.spot(dz, i, j)
        return {"pair": z * self.side + y, "aux": x * 2 + self.core}

    def partner(self):
        return {"pair": self.z * self.side + self.y, "aux": self.x * 2 + 1 - self.core}

    def peers(self):
        found = [self.device(dz, 0, 0) for dz in range(1, self.deep)]
        found += [self.device(0, i, 0) for i in range(1, self.side)]
        found += [self.device(0, 0, j) for j in range(1, self.side)]
        return found + [self.partner()]

    def greet(self):
        barrier = pltpu.get_barrier_semaphore()
        peers = self.peers()
        for peer in peers:
            pl.semaphore_signal(barrier, inc=1, device_id=peer, device_id_type=pl.DeviceIdType.MESH)
        pl.semaphore_wait(barrier, len(peers))


class Sender:
    def __init__(self, sems):
        self.sems, self.started = sems, []

    def send(self, source, target, arrival, device):
        copy = pltpu.make_async_remote_copy(
            src_ref=source,
            dst_ref=target,
            send_sem=self.sems.at[len(self.started)],
            recv_sem=arrival,
            device_id=device,
            device_id_type=pl.DeviceIdType.MESH,
        )
        copy.start()
        self.started.append(copy)

    def arrived(self, target, arrival, device):
        pltpu.make_async_remote_copy(
            src_ref=target,
            dst_ref=target,
            send_sem=self.sems.at[0],
            recv_sem=arrival,
            device_id=device,
            device_id_type=pl.DeviceIdType.MESH,
        ).wait_recv()

    def finish(self):
        for copy in self.started:
            copy.wait_send()


def gather_kernel(pairs, aux, own_ref, out_ref, send_sem, recv_sem, local_sem):
    here = Place(pairs, aux)
    deep, side = here.deep, here.side
    out = Sender(send_sem)
    keep = pltpu.make_async_copy(own_ref, out_ref.at[here.block(0, 0, 0)], local_sem)
    keep.start()
    here.greet()

    def forward(dz, i, j, source):
        block = here.block(dz, i, j)
        target, arrival = out_ref.at[block], recv_sem.at[block]
        if j == 0:
            for step in range(1, side):
                out.send(source, target, arrival, here.device(0, 0, step))
        if i == 0 and j == 0:
            for step in range(1, side):
                out.send(source, target, arrival, here.device(0, step, 0))
        if dz == 0 and i == 0 and j == 0:
            for step in range(1, deep):
                out.send(source, target, arrival, here.device(step, 0, 0))
        out.send(source, target, arrival, here.partner())

    def pass_on(dz, i, j):
        block = here.block(dz, i, j)
        out.arrived(out_ref.at[block], recv_sem.at[block], here.partner())
        forward(dz, i, j, out_ref.at[block])

    forward(0, 0, 0, own_ref)
    for dz in range(deep):
        if dz:
            pass_on(dz, 0, 0)
        for i in range(1, side):
            pass_on(dz, i, 0)
    for dz in range(deep):
        for i in range(side):
            for j in range(1, side):
                pass_on(dz, i, j)
    for dz in range(deep):
        for i in range(side):
            for j in range(side):
                z, y, x = here.spot(dz, i, j)
                block = ((z * side + y) * side + x) * 2 + 1 - here.core
                out.arrived(out_ref.at[block], recv_sem.at[block], here.partner())
    out.finish()
    keep.wait()


def gather(own, pairs, aux):
    blocks = pairs * aux
    return pl.pallas_call(
        functools.partial(gather_kernel, pairs, aux),
        in_specs=[pl.BlockSpec(memory_space=pltpu.VMEM)],
        out_specs=pl.BlockSpec(memory_space=pltpu.VMEM),
        out_shape=jax.ShapeDtypeStruct((blocks,) + own.shape, own.dtype),
        scratch_shapes=[
            pltpu.SemaphoreType.DMA((blocks,)),
            pltpu.SemaphoreType.DMA((blocks,)),
            pltpu.SemaphoreType.DMA,
        ],
        compiler_params=pltpu.CompilerParams(collective_id=0, has_side_effects=True, vmem_limit_bytes=48 << 20),
        name="gather",
    )(own)


def scatter_kernel(
    pairs, aux, part_ref, out_ref, held, mate, third, second, last, third_out, second_out, last_out,
    send_sem, mate_sem, third_sem, second_sem, last_sem,
):
    here = Place(pairs, aux)
    deep, side = here.deep, here.side
    out = Sender(send_sem)
    here.greet()
    order = [*range(1, deep), 0]
    inner = [*range(1, side), 0]

    def spatial(dz, i, j):
        z, y, x = here.spot(dz, i, j)
        return (z * side + y) * side + x

    for group in (range(1, side), range(1)):
        for dz in order:
            for j in inner:
                for i in group:
                    place = spatial(dz, i, j)
                    out.send(part_ref.at[place * 2 + 1 - here.core], mate.at[place], mate_sem.at[place], here.partner())

    def joined(dz, i, j):
        place = spatial(dz, i, j)
        out.arrived(mate.at[place], mate_sem.at[place], here.partner())
        return part_ref[place * 2 + here.core].astype(jnp.float32) + mate[place].astype(jnp.float32)

    for dz in order:
        for i in inner:
            for j in range(1, side):
                slot = (dz * side + i) * (side - 1) + j - 1
                third_out[slot] = joined(dz, i, j).astype(third_out.dtype)
                out.send(third_out.at[slot], third.at[slot], third_sem.at[slot], here.device(0, 0, j))
    for dz in order:
        for i in inner:
            held[dz * side + i] = joined(dz, i, 0)

    def sum_third(dz, i):
        total = held[dz * side + i]
        for j in range(1, side):
            slot = (dz * side + i) * (side - 1) + j - 1
            out.arrived(third.at[slot], third_sem.at[slot], here.partner())
            total = total + third[slot].astype(jnp.float32)
        return total

    def sum_second(dz):
        total = held[dz * side]
        for i in range(1, side):
            slot = dz * (side - 1) + i - 1
            out.arrived(second.at[slot], second_sem.at[slot], here.partner())
            total = total + second[slot].astype(jnp.float32)
        return total

    def send_last(dz):
        last_out[dz - 1] = sum_second(dz).astype(last_out.dtype)
        out.send(last_out.at[dz - 1], last.at[dz - 1], last_sem.at[dz - 1], here.device(dz, 0, 0))

    for turn, dz in enumerate(order):
        for i in range(1, side):
            slot = dz * (side - 1) + i - 1
            second_out[slot] = sum_third(dz, i).astype(second_out.dtype)
            out.send(second_out.at[slot], second.at[slot], second_sem.at[slot], here.device(0, i, 0))
        held[dz * side] = sum_third(dz, 0)
        if turn:
            send_last(order[turn - 1])
    total = sum_second(0)
    for dz in range(1, deep):
        out.arrived(last.at[dz - 1], last_sem.at[dz - 1], here.partner())
        total = total + last[dz - 1].astype(jnp.float32)
    out_ref[...] = total
    out.finish()


def scatter(parts, pairs, aux):
    blocks = pairs * aux
    deep, side, _ = layout_of(pairs, aux)
    shape, kind = parts.shape[1:], parts.dtype
    counts = {
        "mate": blocks // 2,
        "third": deep * side * (side - 1),
        "second": deep * (side - 1),
        "last": deep - 1,
    }
    thirds, seconds, lasts = (max(1, counts[name]) for name in ("third", "second", "last"))
    return pl.pallas_call(
        functools.partial(scatter_kernel, pairs, aux),
        in_specs=[pl.BlockSpec(memory_space=pltpu.VMEM)],
        out_specs=pl.BlockSpec(memory_space=pltpu.VMEM),
        out_shape=jax.ShapeDtypeStruct(shape, jnp.float32),
        scratch_shapes=[
            pltpu.VMEM((deep * side,) + shape, jnp.float32),
            pltpu.VMEM((counts["mate"],) + shape, kind),
            pltpu.VMEM((thirds,) + shape, kind),
            pltpu.VMEM((seconds,) + shape, kind),
            pltpu.VMEM((lasts,) + shape, kind),
            pltpu.VMEM((thirds,) + shape, kind),
            pltpu.VMEM((seconds,) + shape, kind),
            pltpu.VMEM((lasts,) + shape, kind),
            pltpu.SemaphoreType.DMA((blocks,)),
            pltpu.SemaphoreType.DMA((counts["mate"],)),
            pltpu.SemaphoreType.DMA((thirds,)),
            pltpu.SemaphoreType.DMA((seconds,)),
            pltpu.SemaphoreType.DMA((lasts,)),
        ],
        compiler_params=pltpu.CompilerParams(collective_id=1, has_side_effects=True, vmem_limit_bytes=56 << 20),
        name="scatter",
    )(parts)


def body(pairs, aux, ints_ac, slot_pair, amplitudes, ranks, pair_occ, pno_energy, occ_energy):
    width = pno_energy.shape[1]
    local = amplitudes.shape[0]
    positions = jnp.arange(width, dtype=jnp.int32)
    masks = (positions[None, :] < ranks[:, None]).astype(jnp.float32)
    square = masks[:, :, None] * masks[:, None, :]
    masked_t = amplitudes.astype(jnp.float32).reshape(local, 2, width, width) * square[:, None]
    own = masked_t.astype(jnp.bfloat16).transpose(0, 2, 1, 3).reshape(local, width, 2 * width)
    every = gather(own, pairs, aux).reshape(-1, width, 2 * width)
    out = partials(ints_ac, slot_pair, every)
    summed = scatter(out.reshape(-1, local, width, 2 * width), pairs, aux)
    source = (positions % 2) * (width // 2) + positions // 2
    place = (positions[:, None] == source[None, :]).astype(jnp.float32)
    split = summed.reshape(local, width, 2, width)
    residual = jnp.einsum(
        "jykx,xa,yb->jkab", split, place, place, precision=lax.Precision.HIGHEST
    )
    residual = residual * square[:, None]
    onehot = (
        pair_occ[:, :, None] == jnp.arange(occ_energy.shape[0], dtype=jnp.int32)[None, None, :]
    ).astype(jnp.float32)
    occ_pair = jnp.einsum("jko,o->jk", onehot, occ_energy, precision=lax.Precision.HIGHEST)
    denom = (
        pno_energy[:, :, None]
        + pno_energy[:, None, :]
        - (occ_pair[:, 0] + occ_pair[:, 1])[:, None, None]
    )
    updated = (masked_t - residual / denom[:, None]) * square[:, None]
    return (
        residual.reshape(local, 2, width * width),
        updated.reshape(local, 2, width * width).astype(jnp.bfloat16),
    )


def solution(mesh):
    placed = (
        P(None, ("pair", "aux"), None),
        P(),
        P(("pair", "aux"), None, None),
        P(("pair", "aux")),
        P(("pair", "aux"), None),
        P(("pair", "aux"), None),
        P(),
    )
    return jax.shard_map(
        functools.partial(body, mesh.shape["pair"], mesh.shape["aux"]),
        mesh=mesh,
        in_specs=placed,
        out_specs=(P(("pair", "aux"), None, None), P(("pair", "aux"), None, None)),
        check_vma=False,
    )
```

```python
import functools

import jax
import jax.numpy as jnp
from jax import lax
from jax.experimental import pallas as pl
from jax.experimental.pallas import tpu as pltpu
from jax.sharding import PartitionSpec as P

CHUNKS = 8


def exchange(load, amps, rows_ref):
    width, lanes = amps.shape
    chunks = width * width // lanes
    aux = rows_ref.shape[0] // chunks
    half_t = lax.broadcasted_iota(jnp.int32, (width, lanes), 1) < width
    half_b = lax.broadcasted_iota(jnp.int32, (chunks, lanes), 1) < width
    for chunk in range(chunks):
        rows_ref[pl.ds(chunk * aux, aux), :] = load(chunk).astype(jnp.float32)
    pieces = []
    for pair in range(aux // 2):
        first = rows_ref[pl.ds(2 * pair, chunks, stride=aux), :]
        second = rows_ref[pl.ds(2 * pair + 1, chunks, stride=aux), :]
        crossed = pltpu.roll(jnp.where(half_b, second, first), width, 1)
        even = jnp.where(half_b, first, crossed)
        odd = jnp.where(half_b, crossed, second)
        pieces.append(jnp.concatenate([even, odd], axis=0).astype(jnp.bfloat16))
    stacked = jnp.concatenate(pieces, axis=0)
    amps = amps.astype(jnp.float32)
    turned = pltpu.roll(amps, width, 1)
    none = jnp.zeros_like(amps)
    weights = jnp.concatenate(
        [
            jnp.concatenate([jnp.where(half_t, amps, none), jnp.where(half_t, none, turned)], axis=0),
            jnp.concatenate([jnp.where(half_t, turned, none), jnp.where(half_t, none, amps)], axis=0),
        ],
        axis=1,
    ).astype(jnp.bfloat16)
    inner = jnp.dot(stacked, weights, preferred_element_type=jnp.float32).astype(jnp.bfloat16)
    left = jnp.concatenate(pieces, axis=1)
    right = jnp.concatenate(
        [
            jnp.concatenate(
                [
                    inner[pair * width : (pair + 1) * width, k * lanes : (k + 1) * lanes]
                    for pair in range(aux // 2)
                ],
                axis=1,
            )
            for k in range(2)
        ],
        axis=0,
    )
    return lax.dot_general(left, right, (((1,), (1,)), ((), ())), preferred_element_type=jnp.float32)


def layout_of(pairs, aux):
    side = aux // 2
    if pairs % side:
        side = 1
    return pairs // side, side, aux // side // 2


class Place:
    def __init__(self, pairs, aux):
        self.deep, self.side, _ = layout_of(pairs, aux)
        pair, lane = lax.axis_index("pair"), lax.axis_index("aux")
        self.z, self.y = pair // self.side, pair % self.side
        self.x, self.core = lane // 2, lane % 2

    def spot(self, dz, i, j):
        z = (self.z + dz) % self.deep
        y = (self.y + i * (1 - self.core) + j * self.core) % self.side
        x = (self.x + j * (1 - self.core) + i * self.core) % self.side
        return z, y, x

    def block(self, dz, i, j):
        z, y, x = self.spot(dz, i, j)
        return ((z * self.side + y) * self.side + x) * 2 + self.core

    def mirror(self, dz, i, j):
        z, y, x = self.spot(dz, j, i)
        return ((z * self.side + y) * self.side + x) * 2 + 1 - self.core

    def device(self, dz, i, j):
        z, y, x = self.spot(dz, i, j)
        return {"pair": z * self.side + y, "aux": x * 2 + self.core}

    def partner(self):
        return {"pair": self.z * self.side + self.y, "aux": self.x * 2 + 1 - self.core}

    def peers(self):
        found = [self.device(dz, 0, 0) for dz in range(1, self.deep)]
        found += [self.device(0, i, 0) for i in range(1, self.side)]
        found += [self.device(0, 0, j) for j in range(1, self.side)]
        return found + [self.partner()]

    def greet(self):
        barrier = pltpu.get_barrier_semaphore()
        peers = self.peers()
        for peer in peers:
            pl.semaphore_signal(barrier, inc=1, device_id=peer, device_id_type=pl.DeviceIdType.MESH)
        pl.semaphore_wait(barrier, len(peers))


def copy_to(source, target, sent, arrival, device):
    return pltpu.make_async_remote_copy(
        src_ref=source,
        dst_ref=target,
        send_sem=sent,
        recv_sem=arrival,
        device_id=device,
        device_id_type=pl.DeviceIdType.MESH,
    )


def residual_kernel(
    pairs, aux, order_ref, ints_ref, own_ref, out_ref,
    ints, amps, rows, fresh, given, mate, held, third, third_out, second, second_out, last, last_out,
    ints_sem, keep_sem, recv_sem, fan_sem, hop3_sem, hop2_sem, hopz_sem,
    given_sem, mate_sem, third_sent, third_sem, second_sent, second_sem, last_sent, last_sem,
):
    here = Place(pairs, aux)
    deep, side = here.deep, here.side
    local = own_ref.shape[0]
    lanes = own_ref.shape[2]
    partner = here.partner()
    square = side * side
    count = ints.shape[0]
    each = count // CHUNKS

    def loads():
        for part in range(CHUNKS):
            span = pl.ds(part * each, each)
            yield pltpu.make_async_copy(ints_ref.at[span], ints.at[span], ints_sem.at[part])

    for load in loads():
        load.start()
    keep = pltpu.make_async_copy(own_ref, amps.at[here.block(0, 0, 0)], keep_sem)
    keep.start()
    here.greet()

    def forward(dz, i, j, source=None, to_third=False, to_second=False, to_deep=False):
        block = here.block(dz, i, j)
        target, arrival = amps.at[block], recv_sem.at[block]
        source = target if source is None else source
        family = (dz * side + i) * side + j
        if to_third:
            for step in range(1, side):
                sent = hop3_sem.at[(dz * side + i) * (side - 1) + step - 1]
                copy_to(source, target, sent, arrival, here.device(0, 0, step)).start()
        if to_second:
            for step in range(1, side):
                sent = hop2_sem.at[dz * (side - 1) + step - 1]
                copy_to(source, target, sent, arrival, here.device(0, step, 0)).start()
        if to_deep:
            for step in range(deep - 1, 0, -1):
                copy_to(source, target, hopz_sem.at[step - 1], arrival, here.device(step, 0, 0)).start()
        copy_to(source, target, fan_sem.at[family], arrival, partner).start()

    def arrived(block):
        copy_to(amps.at[block], amps.at[block], fan_sem.at[0], recv_sem.at[block], partner).wait_recv()

    def pass_on(dz, i, j, **where):
        arrived(here.block(dz, i, j))
        forward(dz, i, j, **where)

    forward(0, 0, 0, own_ref, to_third=True, to_second=True, to_deep=True)
    for i in range(1, side):
        pass_on(0, i, 0, to_third=True)
    pass_on(1, 0, 0, to_third=True, to_second=True)
    for i in range(1, side):
        pass_on(1, i, 0, to_third=True)
    for dz in range(2, deep):
        pass_on(dz, 0, 0, to_third=True, to_second=True)
    for i in range(side):
        for j in range(1, side):
            pass_on(1, i, j)
    keep.wait()
    for load in loads():
        load.wait()

    def compute(block, store):
        for slot in range(local):
            pair = order_ref[block * local + slot]
            store(slot, exchange(
                lambda chunk: ints[pair, :, pl.ds(chunk * lanes, lanes)], amps[block, slot], rows.at[slot]
            ))

    def as_float(value):
        return value.astype(jnp.float32)

    def take(target, arrival):
        copy_to(target, target, given_sem.at[0], arrival, partner).wait_recv()
        return as_float(target[...])

    def third_slot(dz, i, j):
        return (dz * side + i) * (side - 1) + j - 1

    def sum_third(dz, i):
        total = held[dz * side + i]
        for j in range(1, side):
            slot = third_slot(dz, i, j)
            total = total + take(third.at[slot], third_sem.at[slot])
        return total

    def sum_second(dz):
        total = held[dz * side]
        for i in range(1, side):
            slot = dz * (side - 1) + i - 1
            total = total + take(second.at[slot], second_sem.at[slot])
        return total

    def send_last(dz):
        slot = dz - 1
        last_out[slot] = sum_second(dz).astype(last_out.dtype)
        copy_to(last_out.at[slot], last.at[slot], last_sent.at[slot], last_sem.at[slot], here.device(dz, 0, 0)).start()

    def step(turn, carry):
        layer, rest = turn // square, turn % square
        dz = (layer + 1) % deep
        following = (layer + 2) % deep
        i, j = side - 1 - rest % side, side - 1 - rest // side

        theirs = here.mirror(dz, i, j)
        arrived(theirs)

        def give(slot, value):
            given[turn, slot] = value.astype(given.dtype)

        compute(theirs, give)
        copy_to(given.at[turn], mate.at[turn], given_sem.at[turn], mate_sem.at[turn], partner).start()

        mine = here.block(dz, i, j)

        def keep_fresh(slot, value):
            fresh[slot] = value

        compute(mine, keep_fresh)

        @pl.when((rest == 0) & (layer < deep - 2))
        def _():
            for step in range(1, side):
                pass_on(following, step, 0, to_third=True)

        @pl.when((rest == square - 2) & (layer < deep - 1))
        def _():
            for a in range(side):
                for b in range(1, side):
                    pass_on(following, a, b)

        @pl.when((rest == 0) & (layer > 0))
        def _():
            send_last(layer)

        fresh[...] = fresh[...] + take(mate.at[turn], mate_sem.at[turn])

        @pl.when(j > 0)
        def _():
            slot = third_slot(dz, i, j)
            third_out[slot] = fresh[...].astype(third_out.dtype)
            copy_to(third_out.at[slot], third.at[slot], third_sent.at[slot], third_sem.at[slot], here.device(0, 0, j)).start()

        @pl.when(j == 0)
        def _():
            held[dz * side + i] = fresh[...]
            total = sum_third(dz, i)
            held[dz * side + i] = total

            @pl.when(i > 0)
            def _():
                slot = dz * (side - 1) + i - 1
                second_out[slot] = total.astype(second_out.dtype)
                copy_to(second_out.at[slot], second.at[slot], second_sent.at[slot], second_sem.at[slot], here.device(0, i, 0)).start()

        return carry

    lax.fori_loop(0, deep * square, step, 0)
    total = sum_second(0)
    for dz in range(1, deep):
        total = total + take(last.at[dz - 1], last_sem.at[dz - 1])
    out_ref[...] = total

    for sems in (fan_sem, hop3_sem, hop2_sem, hopz_sem, given_sem, third_sent, second_sent, last_sent):
        def drain(turn, carry, sems=sems):
            copy_to(given.at[0], mate.at[0], sems.at[turn], mate_sem.at[0], partner).wait_send()
            return carry

        lax.fori_loop(0, sems.shape[0], drain, 0)


def residual_parts(ints_ac, slot_pair, own, pairs, aux):
    blocks = pairs * aux
    deep, side, _ = layout_of(pairs, aux)
    local, width, lanes = own.shape
    count, funcs, _ = ints_ac.shape
    thirds, seconds, lasts = deep * side * (side - 1), deep * (side - 1), deep - 1

    def buffers(number, kind=own.dtype):
        return pltpu.VMEM((number,) + own.shape, kind)

    dma = pltpu.SemaphoreType.DMA
    return pl.pallas_call(
        functools.partial(residual_kernel, pairs, aux),
        in_specs=[
            pl.BlockSpec(memory_space=pltpu.SMEM),
            pl.BlockSpec(memory_space=pl.ANY),
            pl.BlockSpec(memory_space=pltpu.VMEM),
        ],
        out_specs=pl.BlockSpec(memory_space=pltpu.VMEM),
        out_shape=jax.ShapeDtypeStruct(own.shape, jnp.float32),
        scratch_shapes=[
            pltpu.VMEM(ints_ac.shape, ints_ac.dtype),
            buffers(blocks),
            pltpu.VMEM((local, funcs * width // 2, lanes), jnp.float32),
            pltpu.VMEM(own.shape, jnp.float32),
            buffers(blocks // 2),
            buffers(blocks // 2),
            buffers(deep * side, jnp.float32),
            buffers(thirds),
            buffers(thirds),
            buffers(seconds),
            buffers(seconds),
            buffers(lasts),
            buffers(lasts),
            dma((CHUNKS,)),
            dma,
            dma((blocks,)),
            dma((blocks // 2,)),
            dma((thirds,)),
            dma((seconds,)),
            dma((lasts,)),
            dma((blocks // 2,)),
            dma((blocks // 2,)),
            dma((thirds,)),
            dma((thirds,)),
            dma((seconds,)),
            dma((seconds,)),
            dma((lasts,)),
            dma((lasts,)),
        ],
        compiler_params=pltpu.CompilerParams(collective_id=0, has_side_effects=True, vmem_limit_bytes=62 << 20),
        name="residual_parts",
    )(slot_pair, ints_ac, own)


def body(pairs, aux, ints_ac, slot_pair, amplitudes, ranks, pair_occ, pno_energy, occ_energy):
    width = pno_energy.shape[1]
    local = amplitudes.shape[0]
    positions = jnp.arange(width, dtype=jnp.int32)
    masks = (positions[None, :] < ranks[:, None]).astype(jnp.float32)
    square = masks[:, :, None] * masks[:, None, :]
    masked_t = amplitudes.astype(jnp.float32).reshape(local, 2, width, width) * square[:, None]
    own = masked_t.astype(jnp.bfloat16).transpose(0, 2, 1, 3).reshape(local, width, 2 * width)
    summed = residual_parts(ints_ac, slot_pair, own, pairs, aux)
    source = (positions % 2) * (width // 2) + positions // 2
    place = (positions[:, None] == source[None, :]).astype(jnp.float32)
    split = summed.reshape(local, width, 2, width)
    residual = jnp.einsum(
        "jykx,xa,yb->jkab", split, place, place, precision=lax.Precision.HIGHEST
    )
    residual = residual * square[:, None]
    onehot = (
        pair_occ[:, :, None] == jnp.arange(occ_energy.shape[0], dtype=jnp.int32)[None, None, :]
    ).astype(jnp.float32)
    occ_pair = jnp.einsum("jko,o->jk", onehot, occ_energy, precision=lax.Precision.HIGHEST)
    denom = (
        pno_energy[:, :, None]
        + pno_energy[:, None, :]
        - (occ_pair[:, 0] + occ_pair[:, 1])[:, None, None]
    )
    updated = (masked_t - residual / denom[:, None]) * square[:, None]
    return (
        residual.reshape(local, 2, width * width),
        updated.reshape(local, 2, width * width).astype(jnp.bfloat16),
    )


def solution(mesh):
    placed = (
        P(None, ("pair", "aux"), None),
        P(),
        P(("pair", "aux"), None, None),
        P(("pair", "aux")),
        P(("pair", "aux"), None),
        P(("pair", "aux"), None),
        P(),
    )
    return jax.shard_map(
        functools.partial(body, mesh.shape["pair"], mesh.shape["aux"]),
        mesh=mesh,
        in_specs=placed,
        out_specs=(P(("pair", "aux"), None, None), P(("pair", "aux"), None, None)),
        check_vma=False,
    )
```

```python
import functools

import jax
import jax.numpy as jnp
from jax import lax
from jax.experimental import pallas as pl
from jax.experimental.pallas import tpu as pltpu
from jax.sharding import PartitionSpec as P

CHUNKS = 8
GAP = 4
LAG = 4


def spread(load, rows_ref, aux, width):
    lanes = 2 * width
    chunks = width * width // lanes
    stride = aux + GAP
    half = lax.broadcasted_iota(jnp.int32, (chunks, lanes), 1) < width
    for chunk in range(chunks):
        rows_ref[pl.ds(chunk * stride, aux), :] = load(chunk).astype(jnp.float32)
    pieces = []
    for pair in range(aux // 2):
        first = rows_ref[pl.ds(2 * pair, chunks, stride=stride), :]
        second = rows_ref[pl.ds(2 * pair + 1, chunks, stride=stride), :]
        crossed = pltpu.roll(jnp.where(half, second, first), width, 1)
        even = jnp.where(half, first, crossed)
        odd = jnp.where(half, crossed, second)
        pieces.append(jnp.concatenate([even, odd], axis=0).astype(jnp.bfloat16))
    return pieces


def contract(pieces, amps):
    width, lanes = amps.shape
    half = lax.broadcasted_iota(jnp.int32, (width, lanes), 1) < width
    amps = amps.astype(jnp.float32)
    turned = pltpu.roll(amps, width, 1)
    none = jnp.zeros_like(amps)
    weights = jnp.concatenate(
        [
            jnp.concatenate([jnp.where(half, amps, none), jnp.where(half, none, turned)], axis=0),
            jnp.concatenate([jnp.where(half, turned, none), jnp.where(half, none, amps)], axis=0),
        ],
        axis=1,
    ).astype(jnp.bfloat16)
    stacked = jnp.concatenate(pieces, axis=0)
    return jnp.dot(stacked, weights, preferred_element_type=jnp.float32).astype(jnp.bfloat16)


def close(pieces, inner):
    width, lanes = pieces[0].shape
    left = jnp.concatenate(pieces, axis=1)
    right = []
    for index in range(len(pieces)):
        rows = slice(index * width, (index + 1) * width)
        right.append(jnp.concatenate([inner[rows, :lanes], inner[rows, lanes:]], axis=0).T)
    return jnp.dot(left, jnp.concatenate(right, axis=0), preferred_element_type=jnp.float32)


def layout_of(pairs, aux):
    side = aux // 2
    if pairs % side:
        side = 1
    return pairs // side, side, aux // side // 2


class Place:
    def __init__(self, pairs, aux):
        self.deep, self.side, _ = layout_of(pairs, aux)
        pair, lane = lax.axis_index("pair"), lax.axis_index("aux")
        self.z, self.y = pair // self.side, pair % self.side
        self.x, self.core = lane // 2, lane % 2

    def spot(self, dz, i, j):
        z = (self.z + dz) % self.deep
        y = (self.y + i * (1 - self.core) + j * self.core) % self.side
        x = (self.x + j * (1 - self.core) + i * self.core) % self.side
        return z, y, x

    def block(self, dz, i, j):
        z, y, x = self.spot(dz, i, j)
        return ((z * self.side + y) * self.side + x) * 2 + self.core

    def mirror(self, dz, i, j):
        z, y, x = self.spot(dz, j, i)
        return ((z * self.side + y) * self.side + x) * 2 + 1 - self.core

    def device(self, dz, i, j):
        z, y, x = self.spot(dz, i, j)
        return {"pair": z * self.side + y, "aux": x * 2 + self.core}

    def partner(self):
        return {"pair": self.z * self.side + self.y, "aux": self.x * 2 + 1 - self.core}

    def peers(self):
        found = [self.device(dz, 0, 0) for dz in range(1, self.deep)]
        found += [self.device(0, i, 0) for i in range(1, self.side)]
        found += [self.device(0, 0, j) for j in range(1, self.side)]
        return found + [self.partner()]

    def greet(self):
        barrier = pltpu.get_barrier_semaphore()
        peers = self.peers()
        for peer in peers:
            pl.semaphore_signal(barrier, inc=1, device_id=peer, device_id_type=pl.DeviceIdType.MESH)
        pl.semaphore_wait(barrier, len(peers))


def copy_to(source, target, sent, arrival, device):
    return pltpu.make_async_remote_copy(
        src_ref=source,
        dst_ref=target,
        send_sem=sent,
        recv_sem=arrival,
        device_id=device,
        device_id_type=pl.DeviceIdType.MESH,
    )


def residual_kernel(
    pairs, aux, order_ref, ints_ref, own_ref, out_ref,
    ints, amps, rows, fresh, given, mate, held, third, third_out, second, second_out, last, last_out,
    ints_sem, keep_sem, recv_sem, fan_sem, hop3_sem, hop2_sem, hopz_sem,
    given_sem, mate_sem, third_sent, third_sem, second_sent, second_sem, last_sent, last_sem,
):
    here = Place(pairs, aux)
    deep, side = here.deep, here.side
    local = own_ref.shape[0]
    lanes = own_ref.shape[2]
    partner = here.partner()
    square = side * side
    count = ints.shape[0]
    each = count // CHUNKS

    def loads():
        for part in range(CHUNKS):
            span = pl.ds(part * each, each)
            yield pltpu.make_async_copy(ints_ref.at[span], ints.at[span], ints_sem.at[part])

    for load in loads():
        load.start()
    keep = pltpu.make_async_copy(own_ref, amps.at[here.block(0, 0, 0)], keep_sem)
    keep.start()
    here.greet()

    def forward(dz, i, j, source=None, to_third=False, to_second=False, to_deep=False):
        block = here.block(dz, i, j)
        target, arrival = amps.at[block], recv_sem.at[block]
        source = target if source is None else source
        family = (dz * side + i) * side + j
        if to_third:
            for step in range(1, side):
                sent = hop3_sem.at[(dz * side + i) * (side - 1) + step - 1]
                copy_to(source, target, sent, arrival, here.device(0, 0, step)).start()
        if to_second:
            for step in range(1, side):
                sent = hop2_sem.at[dz * (side - 1) + step - 1]
                copy_to(source, target, sent, arrival, here.device(0, step, 0)).start()
        if to_deep:
            for step in range(deep - 1, 0, -1):
                copy_to(source, target, hopz_sem.at[step - 1], arrival, here.device(step, 0, 0)).start()
        copy_to(source, target, fan_sem.at[family], arrival, partner).start()

    def arrived(block):
        copy_to(amps.at[block], amps.at[block], fan_sem.at[0], recv_sem.at[block], partner).wait_recv()

    def pass_on(dz, i, j, **where):
        arrived(here.block(dz, i, j))
        forward(dz, i, j, **where)

    forward(0, 0, 0, own_ref, to_third=True, to_second=True, to_deep=True)
    for i in range(1, side):
        pass_on(0, i, 0, to_third=True)
    pass_on(1, 0, 0, to_third=True, to_second=True)
    for i in range(1, side):
        pass_on(1, i, 0, to_third=True)
    for dz in range(2, deep):
        pass_on(dz, 0, 0, to_third=True, to_second=True)
    for i in range(side):
        for j in range(1, side):
            pass_on(1, i, j)
    keep.wait()
    for load in loads():
        load.wait()

    def compute(jobs):
        waiting = []

        def finish():
            store, pieces, inner = waiting.pop(0)
            store(close(pieces, inner))

        for job, (block, slot, store) in enumerate(jobs):
            pair = order_ref[block * local + slot]
            pieces = spread(
                lambda chunk: ints[pair, :, pl.ds(chunk * lanes, lanes)], rows.at[job], ints.shape[1], lanes // 2
            )
            waiting.append((store, pieces, contract(pieces, amps[block, slot])))
            if len(waiting) > LAG:
                finish()
        while waiting:
            finish()

    def as_float(value):
        return value.astype(jnp.float32)

    def take(target, arrival):
        copy_to(target, target, given_sem.at[0], arrival, partner).wait_recv()
        return as_float(target[...])

    def third_slot(dz, i, j):
        return (dz * side + i) * (side - 1) + j - 1

    def sum_second(dz):
        total = held[dz * side]
        for i in range(1, side):
            slot = dz * (side - 1) + i - 1
            total = total + take(second.at[slot], second_sem.at[slot])
        return total

    def send_last(dz):
        slot = dz - 1
        last_out[slot] = sum_second(dz).astype(last_out.dtype)
        copy_to(last_out.at[slot], last.at[slot], last_sent.at[slot], last_sem.at[slot], here.device(dz, 0, 0)).start()

    def shift_of(turn):
        layer, rest = turn // square, turn % square
        return (layer + 1) % deep, side - 1 - rest % side, side - 1 - rest // side

    def settle(turn):
        dz, i, j = shift_of(turn)
        total = fresh[turn % 2] + take(mate.at[turn], mate_sem.at[turn])

        @pl.when(j > 0)
        def _():
            slot = third_slot(dz, i, j)
            third_out[slot] = total.astype(third_out.dtype)
            copy_to(third_out.at[slot], third.at[slot], third_sent.at[slot], third_sem.at[slot], here.device(0, 0, j)).start()

        @pl.when(j == 0)
        def _():
            whole = total
            for other in range(1, side):
                slot = third_slot(dz, i, other)
                whole = whole + take(third.at[slot], third_sem.at[slot])
            held[dz * side + i] = whole

            @pl.when(i > 0)
            def _():
                slot = dz * (side - 1) + i - 1
                second_out[slot] = whole.astype(second_out.dtype)
                copy_to(second_out.at[slot], second.at[slot], second_sent.at[slot], second_sem.at[slot], here.device(0, i, 0)).start()

    turns = deep * square

    def step(turn, carry):
        layer, rest = turn // square, turn % square
        dz, i, j = shift_of(turn)
        following = (layer + 2) % deep
        theirs, mine = here.mirror(dz, i, j), here.block(dz, i, j)
        arrived(theirs)

        def give(slot):
            def store(value):
                given[turn, slot] = value.astype(given.dtype)

            return store

        def retain(slot):
            def store(value):
                fresh[turn % 2, slot] = value

            return store

        compute(
            [(theirs, slot, give(slot)) for slot in range(local)]
            + [(mine, slot, retain(slot)) for slot in range(local)]
        )
        copy_to(given.at[turn], mate.at[turn], given_sem.at[turn], mate_sem.at[turn], partner).start()

        @pl.when((rest == 0) & (layer < deep - 2))
        def _():
            for hop in range(1, side):
                pass_on(following, hop, 0, to_third=True)

        @pl.when((rest == square - 2) & (layer < deep - 1))
        def _():
            for a in range(side):
                for b in range(1, side):
                    pass_on(following, a, b)

        @pl.when(turn > 0)
        def _():
            settle(turn - 1)

        @pl.when((rest == 1) & (layer > 0))
        def _():
            send_last(layer)

        return carry

    lax.fori_loop(0, turns, step, 0)
    settle(turns - 1)
    total = sum_second(0)
    for dz in range(1, deep):
        total = total + take(last.at[dz - 1], last_sem.at[dz - 1])
    out_ref[...] = total

    for sems in (fan_sem, hop3_sem, hop2_sem, hopz_sem, given_sem, third_sent, second_sent, last_sent):
        def drain(turn, carry, sems=sems):
            copy_to(given.at[0], mate.at[0], sems.at[turn], mate_sem.at[0], partner).wait_send()
            return carry

        lax.fori_loop(0, sems.shape[0], drain, 0)


def residual_parts(ints_ac, slot_pair, own, pairs, aux):
    blocks = pairs * aux
    deep, side, _ = layout_of(pairs, aux)
    local, width, lanes = own.shape
    count, funcs, _ = ints_ac.shape
    thirds, seconds, lasts = deep * side * (side - 1), deep * (side - 1), deep - 1

    def buffers(number, kind=own.dtype):
        return pltpu.VMEM((number,) + own.shape, kind)

    dma = pltpu.SemaphoreType.DMA
    return pl.pallas_call(
        functools.partial(residual_kernel, pairs, aux),
        in_specs=[
            pl.BlockSpec(memory_space=pltpu.SMEM),
            pl.BlockSpec(memory_space=pl.ANY),
            pl.BlockSpec(memory_space=pltpu.VMEM),
        ],
        out_specs=pl.BlockSpec(memory_space=pltpu.VMEM),
        out_shape=jax.ShapeDtypeStruct(own.shape, jnp.float32),
        scratch_shapes=[
            pltpu.VMEM(ints_ac.shape, ints_ac.dtype),
            buffers(blocks),
            pltpu.VMEM((2 * local, (width // 2 + 1) * (funcs + GAP), lanes), jnp.float32),
            buffers(2, jnp.float32),
            buffers(blocks // 2),
            buffers(blocks // 2),
            buffers(deep * side, jnp.float32),
            buffers(thirds),
            buffers(thirds),
            buffers(seconds),
            buffers(seconds),
            buffers(lasts),
            buffers(lasts),
            dma((CHUNKS,)),
            dma,
            dma((blocks,)),
            dma((blocks // 2,)),
            dma((thirds,)),
            dma((seconds,)),
            dma((lasts,)),
            dma((blocks // 2,)),
            dma((blocks // 2,)),
            dma((thirds,)),
            dma((thirds,)),
            dma((seconds,)),
            dma((seconds,)),
            dma((lasts,)),
            dma((lasts,)),
        ],
        compiler_params=pltpu.CompilerParams(collective_id=0, has_side_effects=True, vmem_limit_bytes=62 << 20),
        name="residual_parts",
    )(slot_pair, ints_ac, own)


def body(pairs, aux, ints_ac, slot_pair, amplitudes, ranks, pair_occ, pno_energy, occ_energy):
    width = pno_energy.shape[1]
    local = amplitudes.shape[0]
    positions = jnp.arange(width, dtype=jnp.int32)
    masks = (positions[None, :] < ranks[:, None]).astype(jnp.float32)
    square = masks[:, :, None] * masks[:, None, :]
    masked_t = amplitudes.astype(jnp.float32).reshape(local, 2, width, width) * square[:, None]
    own = masked_t.astype(jnp.bfloat16).transpose(0, 2, 1, 3).reshape(local, width, 2 * width)
    summed = residual_parts(ints_ac, slot_pair, own, pairs, aux)
    source = (positions % 2) * (width // 2) + positions // 2
    place = (positions[:, None] == source[None, :]).astype(jnp.float32)
    split = summed.reshape(local, width, 2, width)
    residual = jnp.einsum(
        "jykx,xa,yb->jkab", split, place, place, precision=lax.Precision.HIGHEST
    )
    residual = residual * square[:, None]
    onehot = (
        pair_occ[:, :, None] == jnp.arange(occ_energy.shape[0], dtype=jnp.int32)[None, None, :]
    ).astype(jnp.float32)
    occ_pair = jnp.einsum("jko,o->jk", onehot, occ_energy, precision=lax.Precision.HIGHEST)
    denom = (
        pno_energy[:, :, None]
        + pno_energy[:, None, :]
        - (occ_pair[:, 0] + occ_pair[:, 1])[:, None, None]
    )
    updated = (masked_t - residual / denom[:, None]) * square[:, None]
    return (
        residual.reshape(local, 2, width * width),
        updated.reshape(local, 2, width * width).astype(jnp.bfloat16),
    )


def solution(mesh):
    placed = (
        P(None, ("pair", "aux"), None),
        P(),
        P(("pair", "aux"), None, None),
        P(("pair", "aux")),
        P(("pair", "aux"), None),
        P(("pair", "aux"), None),
        P(),
    )
    return jax.shard_map(
        functools.partial(body, mesh.shape["pair"], mesh.shape["aux"]),
        mesh=mesh,
        in_specs=placed,
        out_specs=(P(("pair", "aux"), None, None), P(("pair", "aux"), None, None)),
        check_vma=False,
    )
```

```python
import functools
import math

import jax
import jax.numpy as jnp
from jax import lax
from jax.experimental import pallas as pl
from jax.experimental.pallas import tpu as pltpu
from jax.sharding import PartitionSpec as P

CHUNKS = 8
GAP = 4
LAG = 4


def spread(load, rows_ref, aux, width):
    lanes = 2 * width
    chunks = width * width // lanes
    stride = aux + GAP
    half = lax.broadcasted_iota(jnp.int32, (chunks, lanes), 1) < width
    for chunk in range(chunks):
        rows_ref[pl.ds(chunk * stride, aux), :] = load(chunk).astype(jnp.float32)
    pieces = []
    for pair in range(aux // 2):
        first = rows_ref[pl.ds(2 * pair, chunks, stride=stride), :]
        second = rows_ref[pl.ds(2 * pair + 1, chunks, stride=stride), :]
        crossed = pltpu.roll(jnp.where(half, second, first), width, 1)
        even = jnp.where(half, first, crossed)
        odd = jnp.where(half, crossed, second)
        pieces.append(jnp.concatenate([even, odd], axis=0).astype(jnp.bfloat16))
    return pieces


def contract(pieces, amps):
    width, lanes = amps.shape
    half = lax.broadcasted_iota(jnp.int32, (width, lanes), 1) < width
    amps = amps.astype(jnp.float32)
    turned = pltpu.roll(amps, width, 1)
    none = jnp.zeros_like(amps)
    weights = jnp.concatenate(
        [
            jnp.concatenate([jnp.where(half, amps, none), jnp.where(half, none, turned)], axis=0),
            jnp.concatenate([jnp.where(half, turned, none), jnp.where(half, none, amps)], axis=0),
        ],
        axis=1,
    ).astype(jnp.bfloat16)
    stacked = jnp.concatenate(pieces, axis=0)
    return jnp.dot(stacked, weights, preferred_element_type=jnp.float32).astype(jnp.bfloat16)


def close(pieces, inner):
    width, lanes = pieces[0].shape
    left = jnp.concatenate(pieces, axis=1)
    right = []
    for index in range(len(pieces)):
        rows = slice(index * width, (index + 1) * width)
        right.append(jnp.concatenate([inner[rows, :lanes], inner[rows, lanes:]], axis=0).T)
    return jnp.dot(left, jnp.concatenate(right, axis=0), preferred_element_type=jnp.float32)


def layout_of(pairs, aux):
    side = aux // 2
    if pairs % side:
        side = 1
    return pairs // side, side, aux // side // 2


class Place:
    def __init__(self, pairs, aux):
        self.deep, self.side, _ = layout_of(pairs, aux)
        pair, lane = lax.axis_index("pair"), lax.axis_index("aux")
        self.z, self.y = pair // self.side, pair % self.side
        self.x, self.core = lane // 2, lane % 2

    def spot(self, dz, i, j):
        z = (self.z + dz) % self.deep
        y = (self.y + i * (1 - self.core) + j * self.core) % self.side
        x = (self.x + j * (1 - self.core) + i * self.core) % self.side
        return z, y, x

    def block(self, dz, i, j):
        z, y, x = self.spot(dz, i, j)
        return ((z * self.side + y) * self.side + x) * 2 + self.core

    def mirror(self, dz, i, j):
        z, y, x = self.spot(dz, j, i)
        return ((z * self.side + y) * self.side + x) * 2 + 1 - self.core

    def device(self, dz, i, j):
        z, y, x = self.spot(dz, i, j)
        return {"pair": z * self.side + y, "aux": x * 2 + self.core}

    def partner(self):
        return {"pair": self.z * self.side + self.y, "aux": self.x * 2 + 1 - self.core}

    def peers(self):
        found = [self.device(dz, 0, 0) for dz in range(1, self.deep)]
        found += [self.device(0, i, 0) for i in range(1, self.side)]
        found += [self.device(0, 0, j) for j in range(1, self.side)]
        return found + [self.partner()]

    def greet(self):
        barrier = pltpu.get_barrier_semaphore()
        peers = self.peers()
        for peer in peers:
            pl.semaphore_signal(barrier, inc=1, device_id=peer, device_id_type=pl.DeviceIdType.MESH)
        pl.semaphore_wait(barrier, len(peers))


def copy_to(source, target, sent, arrival, device):
    return pltpu.make_async_remote_copy(
        src_ref=source,
        dst_ref=target,
        send_sem=sent,
        recv_sem=arrival,
        device_id=device,
        device_id_type=pl.DeviceIdType.MESH,
    )


def residual_kernel(
    pairs, aux, order_ref, ranks_ref, ints_ref, raw_ref, out_ref,
    ints, amps, plain, rows, fresh, given, mate, held, third, third_out, second, second_out, last, last_out,
    ints_sem, recv_sem, fan_sem, hop3_sem, hop2_sem, hopz_sem,
    given_sem, mate_sem, third_sent, third_sem, second_sent, second_sem, last_sent, last_sem,
):
    here = Place(pairs, aux)
    deep, side = here.deep, here.side
    local, width, lanes = out_ref.shape
    home = amps.at[here.block(0, 0, 0)]
    partner = here.partner()
    square = side * side
    count = ints.shape[0]
    each = count // CHUNKS

    def loads():
        for part in range(CHUNKS):
            span = pl.ds(part * each, each)
            yield pltpu.make_async_copy(ints_ref.at[span], ints.at[span], ints_sem.at[part])

    for load in loads():
        load.start()
    for slot in range(local):
        natural(raw_ref, slot, plain.at[0])
        half = width // 2
        zero, one = plain[0, :half], plain[0, half:]
        low = lax.broadcasted_iota(jnp.int32, (half, lanes), 1) < width
        crossed = pltpu.roll(jnp.where(low, one, zero), width, 1)
        plain[1, pl.ds(0, half, stride=2), :] = jnp.where(low, zero, crossed)
        plain[1, pl.ds(1, half, stride=2), :] = jnp.where(low, crossed, one)
        row = lax.broadcasted_iota(jnp.int32, (width, lanes), 0)
        column = lax.broadcasted_iota(jnp.int32, (width, lanes), 1) % width
        inside = (row < ranks_ref[slot]) & (column < ranks_ref[slot])
        home[slot] = jnp.where(inside, plain[1], 0.0).astype(home.dtype)
    here.greet()

    def forward(dz, i, j, to_third=False, to_second=False, to_deep=False):
        block = here.block(dz, i, j)
        target, arrival = amps.at[block], recv_sem.at[block]
        source = target
        family = (dz * side + i) * side + j
        if to_third:
            for step in range(1, side):
                sent = hop3_sem.at[(dz * side + i) * (side - 1) + step - 1]
                copy_to(source, target, sent, arrival, here.device(0, 0, step)).start()
        if to_second:
            for step in range(1, side):
                sent = hop2_sem.at[dz * (side - 1) + step - 1]
                copy_to(source, target, sent, arrival, here.device(0, step, 0)).start()
        if to_deep:
            for step in range(deep - 1, 0, -1):
                copy_to(source, target, hopz_sem.at[step - 1], arrival, here.device(step, 0, 0)).start()
        copy_to(source, target, fan_sem.at[family], arrival, partner).start()

    def arrived(block):
        copy_to(amps.at[block], amps.at[block], fan_sem.at[0], recv_sem.at[block], partner).wait_recv()

    def pass_on(dz, i, j, **where):
        arrived(here.block(dz, i, j))
        forward(dz, i, j, **where)

    forward(0, 0, 0, to_third=True, to_second=True, to_deep=True)
    for i in range(1, side):
        pass_on(0, i, 0, to_third=True)
    pass_on(1, 0, 0, to_third=True, to_second=True)
    for i in range(1, side):
        pass_on(1, i, 0, to_third=True)
    for dz in range(2, deep):
        pass_on(dz, 0, 0, to_third=True, to_second=True)
    for i in range(side):
        for j in range(1, side):
            pass_on(1, i, j)
    for load in loads():
        load.wait()

    def compute(jobs):
        waiting = []

        def finish():
            store, pieces, inner = waiting.pop(0)
            store(close(pieces, inner))

        for job, (block, slot, store) in enumerate(jobs):
            pair = order_ref[block * local + slot]
            pieces = spread(
                lambda chunk: ints[pair, :, pl.ds(chunk * lanes, lanes)], rows.at[job], ints.shape[1], lanes // 2
            )
            waiting.append((store, pieces, contract(pieces, amps[block, slot])))
            if len(waiting) > LAG:
                finish()
        while waiting:
            finish()

    def as_float(value):
        return value.astype(jnp.float32)

    def take(target, arrival):
        copy_to(target, target, given_sem.at[0], arrival, partner).wait_recv()
        return as_float(target[...])

    def third_slot(dz, i, j):
        return (dz * side + i) * (side - 1) + j - 1

    def sum_second(dz):
        total = held[dz * side]
        for i in range(1, side):
            slot = dz * (side - 1) + i - 1
            total = total + take(second.at[slot], second_sem.at[slot])
        return total

    def send_last(dz):
        slot = dz - 1
        last_out[slot] = sum_second(dz).astype(last_out.dtype)
        copy_to(last_out.at[slot], last.at[slot], last_sent.at[slot], last_sem.at[slot], here.device(dz, 0, 0)).start()

    def shift_of(turn):
        layer, rest = turn // square, turn % square
        return (layer + 1) % deep, side - 1 - rest % side, side - 1 - rest // side

    def settle(turn):
        dz, i, j = shift_of(turn)
        total = fresh[turn % 2] + take(mate.at[turn], mate_sem.at[turn])

        @pl.when(j > 0)
        def _():
            slot = third_slot(dz, i, j)
            third_out[slot] = total.astype(third_out.dtype)
            copy_to(third_out.at[slot], third.at[slot], third_sent.at[slot], third_sem.at[slot], here.device(0, 0, j)).start()

        @pl.when(j == 0)
        def _():
            whole = total
            for other in range(1, side):
                slot = third_slot(dz, i, other)
                whole = whole + take(third.at[slot], third_sem.at[slot])
            held[dz * side + i] = whole

            @pl.when(i > 0)
            def _():
                slot = dz * (side - 1) + i - 1
                second_out[slot] = whole.astype(second_out.dtype)
                copy_to(second_out.at[slot], second.at[slot], second_sent.at[slot], second_sem.at[slot], here.device(0, i, 0)).start()

    turns = deep * square

    def step(turn, carry):
        layer, rest = turn // square, turn % square
        dz, i, j = shift_of(turn)
        following = (layer + 2) % deep
        theirs, mine = here.mirror(dz, i, j), here.block(dz, i, j)
        arrived(theirs)

        def give(slot):
            def store(value):
                given[turn, slot] = value.astype(given.dtype)

            return store

        def retain(slot):
            def store(value):
                fresh[turn % 2, slot] = value

            return store

        compute(
            [(theirs, slot, give(slot)) for slot in range(local)]
            + [(mine, slot, retain(slot)) for slot in range(local)]
        )
        copy_to(given.at[turn], mate.at[turn], given_sem.at[turn], mate_sem.at[turn], partner).start()

        @pl.when((rest == 0) & (layer < deep - 2))
        def _():
            for hop in range(1, side):
                pass_on(following, hop, 0, to_third=True)

        @pl.when((rest == square - 2) & (layer < deep - 1))
        def _():
            for a in range(side):
                for b in range(1, side):
                    pass_on(following, a, b)

        @pl.when(turn > 0)
        def _():
            settle(turn - 1)

        @pl.when((rest == 1) & (layer > 0))
        def _():
            send_last(layer)

        return carry

    lax.fori_loop(0, turns, step, 0)
    settle(turns - 1)
    total = sum_second(0)
    for dz in range(1, deep):
        total = total + take(last.at[dz - 1], last_sem.at[dz - 1])
    out_ref[...] = total

    for sems in (fan_sem, hop3_sem, hop2_sem, hopz_sem, given_sem, third_sent, second_sent, last_sent):
        def drain(turn, carry, sems=sems):
            copy_to(given.at[0], mate.at[0], sems.at[turn], mate_sem.at[0], partner).wait_send()
            return carry

        lax.fori_loop(0, sems.shape[0], drain, 0)


def residual_parts(ints_ac, slot_pair, amplitudes, ranks, pairs, aux):
    blocks = pairs * aux
    deep, side, _ = layout_of(pairs, aux)
    count, funcs, size = ints_ac.shape
    width = math.isqrt(size)
    lanes = 2 * width
    local = amplitudes.shape[0]
    shape = (local, width, lanes)
    thirds, seconds, lasts = deep * side * (side - 1), deep * (side - 1), deep - 1

    def buffers(number, kind=amplitudes.dtype):
        return pltpu.VMEM((number,) + shape, kind)

    dma = pltpu.SemaphoreType.DMA
    return pl.pallas_call(
        functools.partial(residual_kernel, pairs, aux),
        in_specs=[
            pl.BlockSpec(memory_space=pltpu.SMEM),
            pl.BlockSpec(memory_space=pltpu.SMEM),
            pl.BlockSpec(memory_space=pl.ANY),
            pl.BlockSpec(memory_space=pltpu.VMEM),
        ],
        out_specs=pl.BlockSpec(memory_space=pltpu.VMEM),
        out_shape=jax.ShapeDtypeStruct(shape, jnp.float32),
        scratch_shapes=[
            pltpu.VMEM(ints_ac.shape, ints_ac.dtype),
            buffers(blocks),
            pltpu.VMEM((2, width, lanes), jnp.float32),
            pltpu.VMEM((2 * local, (width // 2 + 1) * (funcs + GAP), lanes), jnp.float32),
            buffers(2, jnp.float32),
            buffers(blocks // 2),
            buffers(blocks // 2),
            buffers(deep * side, jnp.float32),
            buffers(thirds),
            buffers(thirds),
            buffers(seconds),
            buffers(seconds),
            buffers(lasts),
            buffers(lasts),
            dma((CHUNKS,)),
            dma((blocks,)),
            dma((blocks // 2,)),
            dma((thirds,)),
            dma((seconds,)),
            dma((lasts,)),
            dma((blocks // 2,)),
            dma((blocks // 2,)),
            dma((thirds,)),
            dma((thirds,)),
            dma((seconds,)),
            dma((seconds,)),
            dma((lasts,)),
            dma((lasts,)),
        ],
        compiler_params=pltpu.CompilerParams(collective_id=0, has_side_effects=True, vmem_limit_bytes=62 << 20),
        name="residual_parts",
    )(slot_pair, ranks, ints_ac, amplitudes)


def natural(raw_ref, slot, target):
    half, lanes = target.shape[0] // 2, target.shape[1]
    for chunk in range(half):
        target[pl.ds(chunk, 2, stride=half), :] = raw_ref[slot, :, pl.ds(chunk * lanes, lanes)].astype(jnp.float32)


def update_kernel(
    ranks_ref, pair_ref, occ_ref, sum_ref, raw_ref, energy_ref, residual_ref, new_ref, plain, turned, column, packed
):
    local, width, lanes = sum_ref.shape
    half = width // 2
    low = lax.broadcasted_iota(jnp.int32, (half, lanes), 1) < width
    lane = lax.broadcasted_iota(jnp.int32, (half, lanes), 1)
    a = 2 * lax.broadcasted_iota(jnp.int32, (half, lanes), 0) + lane // width
    b = lane % width
    for slot in range(local):
        natural(raw_ref, slot, plain.at[slot])
        turned[slot, pl.ds(0, half, stride=2), :] = sum_ref[slot, :half]
        turned[slot, pl.ds(1, half, stride=2), :] = sum_ref[slot, half:]
        flipped = turned[slot].T
        energy = energy_ref[pl.ds(slot, 1), :]
        along = jnp.concatenate([energy, energy], axis=1)
        column[slot] = jnp.broadcast_to(along, (lanes, lanes)).T
        down = jnp.where(low, column[slot, pl.ds(0, half, stride=2), :], column[slot, pl.ds(1, half, stride=2), :])
        occupied = occ_ref[pair_ref[slot, 0]] + occ_ref[pair_ref[slot, 1]]
        denom = down + along - occupied
        inside = (a < ranks_ref[slot]) & (b < ranks_ref[slot])
        for k in range(2):
            block = flipped[k * width : (k + 1) * width]
            residual = jnp.where(inside, jnp.concatenate([block[:half], block[half:]], axis=1), 0.0)
            kept = jnp.where(inside, plain[slot, k * half : (k + 1) * half], 0.0)
            packed[slot, 0, k * half : (k + 1) * half] = residual
            packed[slot, 1, k * half : (k + 1) * half] = jnp.where(inside, kept - residual / denom, 0.0)
        for chunk in range(half):
            span = pl.ds(chunk * lanes, lanes)
            residual_ref[slot, :, span] = packed[slot, 0, pl.ds(chunk, 2, stride=half), :]
            new_ref[slot, :, span] = packed[slot, 1, pl.ds(chunk, 2, stride=half), :].astype(new_ref.dtype)


def body(pairs, aux, ints_ac, slot_pair, amplitudes, ranks, pair_occ, pno_energy, occ_energy):
    summed = residual_parts(ints_ac, slot_pair, amplitudes, ranks, pairs, aux)
    local, width, lanes = summed.shape
    smem, vmem = pl.BlockSpec(memory_space=pltpu.SMEM), pl.BlockSpec(memory_space=pltpu.VMEM)
    return pl.pallas_call(
        update_kernel,
        in_specs=[smem, smem, smem, vmem, vmem, vmem],
        out_specs=(vmem, vmem),
        out_shape=(
            jax.ShapeDtypeStruct(amplitudes.shape, jnp.float32),
            jax.ShapeDtypeStruct(amplitudes.shape, amplitudes.dtype),
        ),
        scratch_shapes=[
            pltpu.VMEM((local, width, lanes), jnp.float32),
            pltpu.VMEM((local, width, lanes), jnp.float32),
            pltpu.VMEM((local, lanes, lanes), jnp.float32),
            pltpu.VMEM((local, 2, width, lanes), jnp.float32),
        ],
        name="update",
    )(ranks, pair_occ, occ_energy, summed, amplitudes, pno_energy)


def solution(mesh):
    placed = (
        P(None, ("pair", "aux"), None),
        P(),
        P(("pair", "aux"), None, None),
        P(("pair", "aux")),
        P(("pair", "aux"), None),
        P(("pair", "aux"), None),
        P(),
    )
    return jax.shard_map(
        functools.partial(body, mesh.shape["pair"], mesh.shape["aux"]),
        mesh=mesh,
        in_specs=placed,
        out_specs=(P(("pair", "aux"), None, None), P(("pair", "aux"), None, None)),
        check_vma=False,
    )
```

```python
import functools
import math

import jax
import jax.numpy as jnp
from jax import lax
from jax.experimental import pallas as pl
from jax.experimental.pallas import tpu as pltpu
from jax.sharding import PartitionSpec as P

CHUNKS = 8
GAP = 4
LAG = 4


def spread(load, rows_ref, aux, width):
    lanes = 2 * width
    chunks = width * width // lanes
    stride = aux + GAP
    half = lax.broadcasted_iota(jnp.int32, (chunks, lanes), 1) < width
    for chunk in range(chunks):
        rows_ref[pl.ds(chunk * stride, aux), :] = load(chunk).astype(jnp.float32)
    pieces = []
    for pair in range(aux // 2):
        first = rows_ref[pl.ds(2 * pair, chunks, stride=stride), :]
        second = rows_ref[pl.ds(2 * pair + 1, chunks, stride=stride), :]
        crossed = pltpu.roll(jnp.where(half, second, first), width, 1)
        even = jnp.where(half, first, crossed)
        odd = jnp.where(half, crossed, second)
        pieces.append(jnp.concatenate([even, odd], axis=0).astype(jnp.bfloat16))
    return pieces


def contract(pieces, amps):
    width, lanes = amps.shape
    half = lax.broadcasted_iota(jnp.int32, (width, lanes), 1) < width
    amps = amps.astype(jnp.float32)
    turned = pltpu.roll(amps, width, 1)
    none = jnp.zeros_like(amps)
    weights = jnp.concatenate(
        [
            jnp.concatenate([jnp.where(half, amps, none), jnp.where(half, none, turned)], axis=0),
            jnp.concatenate([jnp.where(half, turned, none), jnp.where(half, none, amps)], axis=0),
        ],
        axis=1,
    ).astype(jnp.bfloat16)
    stacked = jnp.concatenate(pieces, axis=0)
    return jnp.dot(stacked, weights, preferred_element_type=jnp.float32).astype(jnp.bfloat16)


def close(pieces, inner):
    width, lanes = pieces[0].shape
    left = jnp.concatenate(pieces, axis=1)
    right = []
    for index in range(len(pieces)):
        rows = slice(index * width, (index + 1) * width)
        right.append(jnp.concatenate([inner[rows, :lanes], inner[rows, lanes:]], axis=0).T)
    return jnp.dot(left, jnp.concatenate(right, axis=0), preferred_element_type=jnp.float32)


def layout_of(pairs, aux):
    side = aux // 2
    if pairs % side:
        side = 1
    return pairs // side, side, aux // side // 2


class Place:
    def __init__(self, pairs, aux):
        self.deep, self.side, _ = layout_of(pairs, aux)
        pair, lane = lax.axis_index("pair"), lax.axis_index("aux")
        self.z, self.y = pair // self.side, pair % self.side
        self.x, self.core = lane // 2, lane % 2

    def spot(self, dz, i, j):
        z = (self.z + dz) % self.deep
        y = (self.y + i * (1 - self.core) + j * self.core) % self.side
        x = (self.x + j * (1 - self.core) + i * self.core) % self.side
        return z, y, x

    def block(self, dz, i, j):
        z, y, x = self.spot(dz, i, j)
        return ((z * self.side + y) * self.side + x) * 2 + self.core

    def mirror(self, dz, i, j):
        z, y, x = self.spot(dz, j, i)
        return ((z * self.side + y) * self.side + x) * 2 + 1 - self.core

    def device(self, dz, i, j):
        z, y, x = self.spot(dz, i, j)
        return {"pair": z * self.side + y, "aux": x * 2 + self.core}

    def partner(self):
        return {"pair": self.z * self.side + self.y, "aux": self.x * 2 + 1 - self.core}

    def peers(self):
        found = [self.device(dz, 0, 0) for dz in range(1, self.deep)]
        found += [self.device(0, i, 0) for i in range(1, self.side)]
        found += [self.device(0, 0, j) for j in range(1, self.side)]
        return found + [self.partner()]

    def greet(self):
        barrier = pltpu.get_barrier_semaphore()
        peers = self.peers()
        for peer in peers:
            pl.semaphore_signal(barrier, inc=1, device_id=peer, device_id_type=pl.DeviceIdType.MESH)
        pl.semaphore_wait(barrier, len(peers))


def copy_to(source, target, sent, arrival, device):
    return pltpu.make_async_remote_copy(
        src_ref=source,
        dst_ref=target,
        send_sem=sent,
        recv_sem=arrival,
        device_id=device,
        device_id_type=pl.DeviceIdType.MESH,
    )


def residual_kernel(
    pairs, aux, order_ref, ranks_ref, ints_ref, raw_ref, out_ref,
    ints, amps, plain, rows, fresh, given, mate, held, third, third_out, second, second_out, last, last_out,
    ints_sem, recv_sem, fan_sem, hop3_sem, hop2_sem, hopz_sem,
    given_sem, mate_sem, third_sent, third_sem, second_sent, second_sem, last_sent, last_sem,
):
    here = Place(pairs, aux)
    deep, side = here.deep, here.side
    local, width, lanes = out_ref.shape
    home = amps.at[here.block(0, 0, 0)]
    partner = here.partner()
    square = side * side
    count = ints.shape[0]
    each = count // CHUNKS

    def loads():
        for part in range(CHUNKS):
            span = pl.ds(part * each, each)
            yield pltpu.make_async_copy(ints_ref.at[span], ints.at[span], ints_sem.at[part])

    for load in loads():
        load.start()
    for slot in range(local):
        natural(raw_ref, slot, plain.at[0])
        half = width // 2
        zero, one = plain[0, :half], plain[0, half:]
        low = lax.broadcasted_iota(jnp.int32, (half, lanes), 1) < width
        crossed = pltpu.roll(jnp.where(low, one, zero), width, 1)
        plain[1, pl.ds(0, half, stride=2), :] = jnp.where(low, zero, crossed)
        plain[1, pl.ds(1, half, stride=2), :] = jnp.where(low, crossed, one)
        row = lax.broadcasted_iota(jnp.int32, (width, lanes), 0)
        column = lax.broadcasted_iota(jnp.int32, (width, lanes), 1) % width
        inside = (row < ranks_ref[slot]) & (column < ranks_ref[slot])
        home[slot] = jnp.where(inside, plain[1], 0.0).astype(home.dtype)
    here.greet()

    def forward(dz, i, j, to_third=False, to_second=False, to_deep=False):
        block = here.block(dz, i, j)
        target, arrival = amps.at[block], recv_sem.at[block]
        source = target
        family = (dz * side + i) * side + j
        if to_third:
            for step in range(1, side):
                sent = hop3_sem.at[(dz * side + i) * (side - 1) + step - 1]
                copy_to(source, target, sent, arrival, here.device(0, 0, step)).start()
        if to_second:
            for step in range(1, side):
                sent = hop2_sem.at[dz * (side - 1) + step - 1]
                copy_to(source, target, sent, arrival, here.device(0, step, 0)).start()
        if to_deep:
            for step in range(deep - 1, 0, -1):
                copy_to(source, target, hopz_sem.at[step - 1], arrival, here.device(step, 0, 0)).start()
        copy_to(source, target, fan_sem.at[family], arrival, partner).start()

    def arrived(block):
        copy_to(amps.at[block], amps.at[block], fan_sem.at[0], recv_sem.at[block], partner).wait_recv()

    def pass_on(dz, i, j, **where):
        arrived(here.block(dz, i, j))
        forward(dz, i, j, **where)

    forward(0, 0, 0, to_third=True, to_second=True, to_deep=True)
    for i in range(1, side):
        pass_on(0, i, 0, to_third=True)
    pass_on(1, 0, 0, to_third=True, to_second=True)
    for i in range(1, side):
        pass_on(1, i, 0, to_third=True)
    for dz in range(2, deep):
        pass_on(dz, 0, 0, to_third=True, to_second=True)
    for i in range(side):
        for j in range(1, side):
            pass_on(1, i, j)
    for load in loads():
        load.wait()

    def compute(jobs):
        waiting = []

        def finish():
            store, pieces, inner = waiting.pop(0)
            store(close(pieces, inner))

        for job, (block, slot, store) in enumerate(jobs):
            pair = order_ref[block * local + slot]
            pieces = spread(
                lambda chunk: ints[pair, :, pl.ds(chunk * lanes, lanes)], rows.at[job], ints.shape[1], lanes // 2
            )
            waiting.append((store, pieces, contract(pieces, amps[block, slot])))
            if len(waiting) > LAG:
                finish()
        while waiting:
            finish()

    def as_float(value):
        return value.astype(jnp.float32)

    def take(target, arrival):
        copy_to(target, target, given_sem.at[0], arrival, partner).wait_recv()
        return as_float(target[...])

    def third_slot(dz, i, j):
        return (dz * side + i) * (side - 1) + j - 1

    def sum_second(dz):
        total = held[dz * side]
        for i in range(1, side):
            slot = dz * (side - 1) + i - 1
            total = total + take(second.at[slot], second_sem.at[slot])
        return total

    def send_last(dz):
        slot = dz - 1
        last_out[slot] = sum_second(dz).astype(last_out.dtype)
        copy_to(last_out.at[slot], last.at[slot], last_sent.at[slot], last_sem.at[slot], here.device(dz, 0, 0)).start()

    def shift_of(turn):
        layer, rest = turn // square, turn % square
        return (layer + 1) % deep, side - 1 - rest % side, side - 1 - rest // side

    def settle(turn):
        dz, i, j = shift_of(turn)
        total = fresh[turn % 2] + take(mate.at[turn], mate_sem.at[turn])

        @pl.when(j > 0)
        def _():
            slot = third_slot(dz, i, j)
            third_out[slot] = total.astype(third_out.dtype)
            copy_to(third_out.at[slot], third.at[slot], third_sent.at[slot], third_sem.at[slot], here.device(0, 0, j)).start()

        @pl.when(j == 0)
        def _():
            whole = total
            for other in range(1, side):
                slot = third_slot(dz, i, other)
                whole = whole + take(third.at[slot], third_sem.at[slot])
            held[dz * side + i] = whole

            @pl.when(i > 0)
            def _():
                slot = dz * (side - 1) + i - 1
                second_out[slot] = whole.astype(second_out.dtype)
                copy_to(second_out.at[slot], second.at[slot], second_sent.at[slot], second_sem.at[slot], here.device(0, i, 0)).start()

    turns = deep * square

    def step(turn, carry):
        layer, rest = turn // square, turn % square
        dz, i, j = shift_of(turn)
        following = (layer + 2) % deep
        theirs, mine = here.mirror(dz, i, j), here.block(dz, i, j)
        arrived(theirs)

        def give(slot):
            def store(value):
                given[turn, slot] = value.astype(given.dtype)

            return store

        def retain(slot):
            def store(value):
                fresh[turn % 2, slot] = value

            return store

        compute(
            [(theirs, slot, give(slot)) for slot in range(local)]
            + [(mine, slot, retain(slot)) for slot in range(local)]
        )
        copy_to(given.at[turn], mate.at[turn], given_sem.at[turn], mate_sem.at[turn], partner).start()

        @pl.when((rest == 0) & (layer < deep - 2))
        def _():
            for hop in range(1, side):
                pass_on(following, hop, 0, to_third=True)

        @pl.when((rest == square - 2) & (layer < deep - 1))
        def _():
            for a in range(side):
                for b in range(1, side):
                    pass_on(following, a, b)

        @pl.when(turn > 0)
        def _():
            settle(turn - 1)

        @pl.when((rest == 1) & (layer > 0))
        def _():
            send_last(layer)

        return carry

    lax.fori_loop(0, turns, step, 0)
    settle(turns - 1)
    total = sum_second(0)
    for dz in range(1, deep):
        total = total + take(last.at[dz - 1], last_sem.at[dz - 1])
    out_ref[...] = total

    for sems in (fan_sem, hop3_sem, hop2_sem, hopz_sem, given_sem, third_sent, second_sent, last_sent):
        def drain(turn, carry, sems=sems):
            copy_to(given.at[0], mate.at[0], sems.at[turn], mate_sem.at[0], partner).wait_send()
            return carry

        lax.fori_loop(0, sems.shape[0], drain, 0)


def residual_parts(ints_ac, slot_pair, amplitudes, ranks, pairs, aux):
    blocks = pairs * aux
    deep, side, _ = layout_of(pairs, aux)
    count, funcs, size = ints_ac.shape
    width = math.isqrt(size)
    lanes = 2 * width
    local = amplitudes.shape[0]
    shape = (local, width, lanes)
    thirds, seconds, lasts = deep * side * (side - 1), deep * (side - 1), deep - 1

    def buffers(number, kind=amplitudes.dtype):
        return pltpu.VMEM((number,) + shape, kind)

    dma = pltpu.SemaphoreType.DMA
    return pl.pallas_call(
        functools.partial(residual_kernel, pairs, aux),
        in_specs=[
            pl.BlockSpec(memory_space=pltpu.SMEM),
            pl.BlockSpec(memory_space=pltpu.SMEM),
            pl.BlockSpec(memory_space=pl.ANY),
            pl.BlockSpec(memory_space=pltpu.VMEM),
        ],
        out_specs=pl.BlockSpec(memory_space=pltpu.VMEM),
        out_shape=jax.ShapeDtypeStruct(shape, jnp.float32),
        scratch_shapes=[
            pltpu.VMEM(ints_ac.shape, ints_ac.dtype),
            buffers(blocks),
            pltpu.VMEM((2, width, lanes), jnp.float32),
            pltpu.VMEM((2 * local, (width // 2 + 1) * (funcs + GAP), lanes), jnp.float32),
            buffers(2, jnp.float32),
            buffers(blocks // 2),
            buffers(blocks // 2),
            buffers(deep * side, jnp.float32),
            buffers(thirds),
            buffers(thirds),
            buffers(seconds),
            buffers(seconds),
            buffers(lasts),
            buffers(lasts),
            dma((CHUNKS,)),
            dma((blocks,)),
            dma((blocks // 2,)),
            dma((thirds,)),
            dma((seconds,)),
            dma((lasts,)),
            dma((blocks // 2,)),
            dma((blocks // 2,)),
            dma((thirds,)),
            dma((thirds,)),
            dma((seconds,)),
            dma((seconds,)),
            dma((lasts,)),
            dma((lasts,)),
        ],
        compiler_params=pltpu.CompilerParams(collective_id=0, has_side_effects=True, vmem_limit_bytes=62 << 20),
        name="residual_parts",
    )(slot_pair, ranks, ints_ac, amplitudes)


def natural(raw_ref, slot, target):
    half, lanes = target.shape[0] // 2, target.shape[1]
    for chunk in range(half):
        target[pl.ds(chunk, 2, stride=half), :] = raw_ref[slot, :, pl.ds(chunk * lanes, lanes)].astype(jnp.float32)


def update_kernel(
    ranks_ref, pair_ref, occ_ref, sum_ref, raw_ref, energy_ref, residual_ref, new_ref, plain, turned, column, packed
):
    local, width, lanes = sum_ref.shape
    half = width // 2
    low = lax.broadcasted_iota(jnp.int32, (half, lanes), 1) < width
    lane = lax.broadcasted_iota(jnp.int32, (half, lanes), 1)
    a = 2 * lax.broadcasted_iota(jnp.int32, (half, lanes), 0) + lane // width
    b = lane % width
    for slot in range(local):
        natural(raw_ref, slot, plain.at[slot])
        turned[slot, pl.ds(0, half, stride=2), :] = sum_ref[slot, :half]
        turned[slot, pl.ds(1, half, stride=2), :] = sum_ref[slot, half:]
        flipped = turned[slot].T
        energy = energy_ref[pl.ds(slot, 1), :]
        along = jnp.concatenate([energy, energy], axis=1)
        column[slot] = jnp.broadcast_to(along, (lanes, lanes)).T
        down = jnp.where(low, column[slot, pl.ds(0, half, stride=2), :], column[slot, pl.ds(1, half, stride=2), :])
        occupied = occ_ref[pair_ref[0, slot]] + occ_ref[pair_ref[1, slot]]
        denom = down + along - occupied
        inside = (a < ranks_ref[slot]) & (b < ranks_ref[slot])
        for k in range(2):
            block = flipped[k * width : (k + 1) * width]
            residual = jnp.where(inside, jnp.concatenate([block[:half], block[half:]], axis=1), 0.0)
            kept = jnp.where(inside, plain[slot, k * half : (k + 1) * half], 0.0)
            packed[slot, 0, k * half : (k + 1) * half] = residual
            packed[slot, 1, k * half : (k + 1) * half] = jnp.where(inside, kept - residual / denom, 0.0)
        for chunk in range(half):
            span = pl.ds(chunk * lanes, lanes)
            residual_ref[slot, :, span] = packed[slot, 0, pl.ds(chunk, 2, stride=half), :]
            new_ref[slot, :, span] = packed[slot, 1, pl.ds(chunk, 2, stride=half), :].astype(new_ref.dtype)


def body(pairs, aux, ints_ac, slot_pair, amplitudes, ranks, pair_occ, pno_energy, occ_energy):
    summed = residual_parts(ints_ac, slot_pair, amplitudes, ranks, pairs, aux)
    local, width, lanes = summed.shape
    smem, vmem = pl.BlockSpec(memory_space=pltpu.SMEM), pl.BlockSpec(memory_space=pltpu.VMEM)
    return pl.pallas_call(
        update_kernel,
        in_specs=[smem, smem, smem, vmem, vmem, vmem],
        out_specs=(vmem, vmem),
        out_shape=(
            jax.ShapeDtypeStruct(amplitudes.shape, jnp.float32),
            jax.ShapeDtypeStruct(amplitudes.shape, amplitudes.dtype),
        ),
        scratch_shapes=[
            pltpu.VMEM((local, width, lanes), jnp.float32),
            pltpu.VMEM((local, width, lanes), jnp.float32),
            pltpu.VMEM((local, lanes, lanes), jnp.float32),
            pltpu.VMEM((local, 2, width, lanes), jnp.float32),
        ],
        name="update",
    )(ranks, pair_occ.T, occ_energy, summed, amplitudes, pno_energy)


def solution(mesh):
    placed = (
        P(None, ("pair", "aux"), None),
        P(),
        P(("pair", "aux"), None, None),
        P(("pair", "aux")),
        P(("pair", "aux"), None),
        P(("pair", "aux"), None),
        P(),
    )
    return jax.shard_map(
        functools.partial(body, mesh.shape["pair"], mesh.shape["aux"]),
        mesh=mesh,
        in_specs=placed,
        out_specs=(P(("pair", "aux"), None, None), P(("pair", "aux"), None, None)),
        check_vma=False,
    )
```
